128 devices in a mesh: dz: 4 (over z), dy: 4 (over y), dx: 8 (over x, core).
Axes of the slice: x: 4, y: 4, z: 4, core: 2. Of those that a mesh axis runs over, the one named last changes fastest.
Arguments:
- g_emb: float32 [128, 2048, 256], P(('dz', 'dy', 'dx'))
- g_attn: float32 [128, 3, 4, 256, 256], P(('dz', 'dy', 'dx'))
- g_in: float32 [128, 3, 256, 1024], P(('dz', 'dy', 'dx'))
- g_out: float32 [128, 3, 1024, 256], P(('dz', 'dy', 'dx'))
- g_vecd: float32 [128, 3, 9, 256], P(('dz', 'dy', 'dx'))
- g_vecf: float32 [128, 3, 1024], P(('dz', 'dy', 'dx'))
- opt_m: float32 [2899968], P(('dz', 'dy', 'dx'))
- opt_v: float32 [2899968], P(('dz', 'dy', 'dx'))
- master: float32 [2899968], P(('dz', 'dy', 'dx'))
- tok_ids: int32 [32768], P(('dz', 'dy', 'dx'))
- act_in: bfloat16 [32768, 256], P(('dz', 'dy', 'dx'))
Outputs:
- output 1: float32 [2899968], P(('dz', 'dy', 'dx'))
- output 2: float32 [2899968], P(('dz', 'dy', 'dx'))
- output 3: float32 [2899968], P(('dz', 'dy', 'dx'))
- output 4: bfloat16 [2048, 256], replicated
- output 5: bfloat16 [3, 4, 256, 256], replicated
- output 6: bfloat16 [3, 256, 1024], replicated
- output 7: bfloat16 [3, 1024, 256], replicated
- output 8: bfloat16 [3, 9, 256], replicated
- output 9: bfloat16 [3, 1024], replicated
- output 10: bfloat16 [32768, 256], P(('dz', 'dy', 'dx'))
All inputs are finite; a program needn't handle non-finite values.
Results may differ from the reference program's by a relative error of at most 0.001.
Values are sent between devices in bfloat16 or wider.
A program may use at most 1 GiB of HBM per device.

```python
import math
import jax
import jax.numpy as jnp
from jax import lax

D = 256
FF = 1024
LAYERS = 3
VOCAB = 2048
TOKENS_DEV = 256
DEVICES = 128
ADAM_STEP = 2

LEARN_RATE = 0.002
BETA_ONE = 0.9
BETA_TWO = 0.95
ADAM_EPS = 1e-8
PARAM_COUNT = VOCAB * D + LAYERS * (4 * D * D + 2 * D * FF + 9 * D + FF)
PADDED_COUNT = -(-PARAM_COUNT // (128 * DEVICES)) * (128 * DEVICES)
TENSOR_SHAPES = [(VOCAB, D), (LAYERS, 4, D, D), (LAYERS, D, FF), (LAYERS, FF, D), (LAYERS, 9, D), (LAYERS, FF)]
ARG_NAMES = ["g_emb", "g_attn", "g_in", "g_out", "g_vecd", "g_vecf"]


def setup_inputs(seed: int = 0) -> dict:
    rand_keys = jax.random.split(jax.random.key(seed), 12)
    dev_scale = jax.random.uniform(rand_keys[0], (DEVICES,), jnp.float32, 0.5, 1.5) * math.sqrt(DEVICES)
    inputs = {}
    for tensor_index, tensor_shape in enumerate(TENSOR_SHAPES):
        grad_noise = jax.random.normal(rand_keys[1 + tensor_index], (DEVICES,) + tensor_shape, jnp.float32)
        inputs[ARG_NAMES[tensor_index]] = grad_noise * dev_scale.reshape((DEVICES,) + (1,) * len(tensor_shape))
    weight_scales = [D ** -0.5, D ** -0.5, D ** -0.5, FF ** -0.5, 0.2, 0.3]
    scale_parts = [jnp.full((math.prod(tensor_shape),), weight_scale, jnp.float32) for tensor_shape, weight_scale in zip(TENSOR_SHAPES, weight_scales)]
    scale_parts.append(jnp.full((PADDED_COUNT - PARAM_COUNT,), 0.1, jnp.float32))
    m_noise = jax.random.normal(rand_keys[7], (PADDED_COUNT,), jnp.float32)
    v_noise = jax.random.normal(rand_keys[8], (PADDED_COUNT,), jnp.float32)
    w_noise = jax.random.normal(rand_keys[9], (PADDED_COUNT,), jnp.float32)
    inputs["opt_m"] = 0.1 * m_noise
    inputs["opt_v"] = 0.05 * (v_noise * v_noise + 0.25)
    inputs["master"] = w_noise * jnp.concatenate(scale_parts)
    tok_ids = jax.random.randint(rand_keys[10], (DEVICES * TOKENS_DEV,), 0, VOCAB, jnp.int32)
    inputs["tok_ids"] = tok_ids.at[0].set(0).at[1].set(VOCAB - 1)
    inputs["act_in"] = jax.random.normal(rand_keys[11], (DEVICES * TOKENS_DEV, D), jnp.float32).astype(jnp.bfloat16)
    return inputs


def ffn_block(wb_emb, w_in, b_in, w_out, b_out, tok_ids, act_in):
    emb_rows = jnp.take(wb_emb, tok_ids, axis=0).astype(jnp.float32)
    hidden = (emb_rows * math.sqrt(D) + act_in.astype(jnp.float32)).astype(jnp.bfloat16)
    pre_act = jnp.dot(hidden, w_in, preferred_element_type=jnp.float32) + b_in.astype(jnp.float32)
    inner_act = jax.nn.gelu(pre_act, approximate=True).astype(jnp.bfloat16)
    return (jnp.dot(inner_act, w_out, preferred_element_type=jnp.float32) + b_out.astype(jnp.float32)).astype(jnp.bfloat16)


def reference(g_emb, g_attn, g_in, g_out, g_vecd, g_vecf, opt_m, opt_v, master, tok_ids, act_in):
    grad_list = [g_emb, g_attn, g_in, g_out, g_vecd, g_vecf]
    flat_grad = jnp.concatenate([jnp.sum(grad_arr, axis=0).reshape(-1) for grad_arr in grad_list]) / DEVICES
    flat_grad = jnp.pad(flat_grad, (0, PADDED_COUNT - PARAM_COUNT))
    m_new = BETA_ONE * opt_m + (1.0 - BETA_ONE) * flat_grad
    v_new = BETA_TWO * opt_v + (1.0 - BETA_TWO) * flat_grad * flat_grad
    m_hat = m_new / (1.0 - BETA_ONE ** ADAM_STEP)
    v_hat = v_new / (1.0 - BETA_TWO ** ADAM_STEP)
    w_new = master - LEARN_RATE * m_hat / (jnp.sqrt(v_hat) + ADAM_EPS)
    w_half = w_new.astype(jnp.bfloat16)
    pieces = []
    offset = 0
    for tensor_shape in TENSOR_SHAPES:
        elem_count = math.prod(tensor_shape)
        pieces.append(w_half[offset:offset + elem_count].reshape(tensor_shape))
        offset = offset + elem_count
    wb_emb, wb_attn, wb_in, wb_out, wb_vecd, wb_vecf = pieces
    tok_blocks = tok_ids.reshape(DEVICES, TOKENS_DEV)
    act_blocks = act_in.reshape(DEVICES, TOKENS_DEV, D)

    def token_block(tok_pair):
        return ffn_block(wb_emb, wb_in[0], wb_vecf[0], wb_out[0], wb_vecd[0, 8], tok_pair[0], tok_pair[1])

    y_blocks = lax.map(token_block, (tok_blocks, act_blocks))
    y_out = y_blocks.reshape(DEVICES * TOKENS_DEV, D)
    return (m_new, v_new, w_new, wb_emb, wb_attn, wb_in, wb_out, wb_vecd, wb_vecf, y_out)
```

```python
import functools
import math
import jax
import jax.numpy as jnp
from jax import lax
from jax.experimental import pallas as pl
from jax.experimental.pallas import tpu as pltpu
from jax.sharding import PartitionSpec as P

LEARN_RATE = 0.002
BETA_ONE = 0.9
BETA_TWO = 0.95
ADAM_EPS = 1e-8
ADAM_STEP = 2
AXES = ("dz", "dy", "dx")
GRAD_RANKS = (3, 5, 4, 4, 4, 3)
MESH = pl.DeviceIdType.MESH

SHARD = 177
PART = 59
APART = 60
ROWS = 22656
REAL = 22606
BASE = (0, 4096, 10240, 16384, 22528, 22582)
GROUPS = (256, 384, 96, 384)
TILES = (2, 2, 8, 2)
ORDER = ((0, 1, 2), (1, 2, 0), (2, 0, 1))
F32 = jnp.float32
BF16 = jnp.bfloat16


def loop(count, body, unroll=1):
    def step(i, carry):
        body(i)
        return carry
    lax.fori_loop(0, count, step, 0, unroll=unroll)


def shard_of(k, q1, q2, q3, core):
    pos = [None] * 3
    for axis, q in zip(ORDER[k], (q1, q2, q3)):
        pos[axis] = q
    return pos[2] * 32 + pos[1] * 8 + pos[0] * 2 + core


def sync_kernel(e_hbm, a_hbm, i_hbm, o_hbm, vd_hbm, vf_hbm, m_ref, v_ref, w_ref,
                m_out, v_out, w_out, ag,
                e_raw, a_raw, i_raw, o_raw, vd_raw, vf_raw, flat, psl, work, drx,
                r1, r2, r3,
                raw_sem, dsend, drecv, ssend, srecv, asend, arecv, gsend, grecv):
    dz, dy, dx = lax.axis_index("dz"), lax.axis_index("dy"), lax.axis_index("dx")
    core = lax.rem(dx, 2)
    pos = (lax.div(dx, 2), dy, dz)
    partner = {"dz": dz, "dy": dy, "dx": dx + 1 - 2 * core}

    def neighbour(axis, shift):
        q = lax.rem(pos[axis] + 4 + shift, 4)
        if axis == 0:
            return {"dz": dz, "dy": dy, "dx": q * 2 + core}
        if axis == 1:
            return {"dz": dz, "dy": q, "dx": dx}
        return {"dz": q, "dy": dy, "dx": dx}

    def ring(axis, shift):
        return lax.rem(pos[axis] + 4 + shift, 4)

    barrier = pltpu.get_barrier_semaphore()
    for axis in range(3):
        for shift in (1, -1):
            pl.semaphore_signal(barrier, inc=1, device_id=neighbour(axis, shift), device_id_type=MESH)
    pl.semaphore_signal(barrier, inc=1, device_id=partner, device_id_type=MESH)

    raws = (e_raw, a_raw, i_raw, o_raw, vd_raw, vf_raw)
    loads = [pltpu.make_async_copy(src, dst, raw_sem.at[n]) for n, (src, dst) in enumerate(
        zip((e_hbm, a_hbm, i_hbm, o_hbm, vd_hbm, vf_hbm), raws))]
    for n in (0, 1, 2, 3, 4, 5):
        loads[n].start()

    flat[pl.ds(REAL, ROWS - REAL), :] = jnp.zeros((ROWS - REAL, 128), F32)
    for n in range(4):
        loads[n].wait()
        tiles, base, raw = TILES[n], BASE[n], raws[n]

        def relayout(g, tiles=tiles, base=base, raw=raw):
            for c in range(tiles):
                flat[pl.ds(base + g * (8 * tiles) + c, 8, stride=tiles), :] = raw[g, c]
        loop(GROUPS[n], relayout, unroll=16 // tiles)
    loads[4].wait()
    flat[pl.ds(BASE[4], 54), :] = vd_raw[...]
    loads[5].wait()
    flat[pl.ds(BASE[5], 24), :] = vf_raw[...]

    pl.semaphore_wait(barrier, 7)

    def flat_row(k, q1, j, c):
        return SHARD * shard_of(k, q1, lax.div(j, 4), lax.rem(j, 4), c) + PART * k

    def d2d(k, q1):
        return pltpu.make_async_remote_copy(
            src_ref=psl.at[k, q1], dst_ref=drx.at[k, q1],
            send_sem=dsend.at[k, q1], recv_sem=drecv.at[k, q1],
            device_id=partner, device_id_type=MESH)

    for shift in (2, 1, -1, 0):
        for k in range(3):
            q1 = ring(ORDER[k][0], shift)

            def pick(j, k=k, q1=q1):
                psl[k, q1, j] = flat[pl.ds(flat_row(k, q1, j, 1 - core), PART), :]
            loop(16, pick, unroll=2)
            d2d(k, q1).start()

    def add_core(k, shift):
        q1 = ring(ORDER[k][0], shift)
        d2d(k, q1).wait_recv()

        def body(j):
            work[k, q1, j] = flat[pl.ds(flat_row(k, q1, j, core), PART), :] + drx[k, q1, j]
        loop(16, body, unroll=2)

    def chunk(t, k, shift, half):
        p = [pos[a] for a in ORDER[k]]
        q = ring(ORDER[k][t], shift)
        if t == 0:
            return work.at[k, q, pl.ds(8 * half, 8)]
        if t == 1:
            return work.at[k, p[0], pl.ds(4 * q + 2 * half, 2)]
        return work.at[k, p[0], 4 * p[1] + q, pl.ds(32 * half, 32 - 5 * half)]

    def landing(t, k, part, half):
        if t == 0:
            return r1.at[k, part]
        if t == 1:
            return r2.at[k, part]
        return r3.at[k, part, pl.ds(0, 32 - 5 * half)]

    PARTS = ((2, 0, 1), (2, 1, -1), (1, 1, 1), (1, 0, 1), (-1, 0, -1), (-1, 1, -1))

    def rs(t, k, part):
        shift, half, way = PARTS[part]
        return pltpu.make_async_remote_copy(
            src_ref=chunk(t, k, shift, half), dst_ref=landing(t, k, part, half),
            send_sem=ssend.at[t, k, part], recv_sem=srecv.at[t, k, part],
            device_id=neighbour(ORDER[k][t], way), device_id_type=MESH)

    def accumulate(t, k, shift, half, part):
        rs(t, k, part).wait_recv()
        dst = chunk(t, k, shift, half)
        src = landing(t, k, part, half)
        if t == 0:
            def body(j):
                dst[j] = dst[j] + src[j]
            loop(8, body, unroll=2)
        else:
            dst[...] = dst[...] + src[...]

    colours = range(3)
    for t in range(3):
        if t == 0:
            for k in colours:
                add_core(k, 2)
                rs(t, k, 0).start()
                rs(t, k, 1).start()
            for k in colours:
                add_core(k, 1)
                rs(t, k, 2).start()
                add_core(k, -1)
                rs(t, k, 4).start()
        else:
            for k in colours:
                rs(t, k, 0).start()
                rs(t, k, 1).start()
                rs(t, k, 2).start()
                rs(t, k, 4).start()
        for k in colours:
            accumulate(t, k, 1, 0, 0)
            rs(t, k, 3).start()
            accumulate(t, k, -1, 1, 1)
            rs(t, k, 5).start()
        if t == 0:
            for k in colours:
                add_core(k, 0)
        for k in colours:
            accumulate(t, k, 0, 1, 2)
            accumulate(t, k, 0, 0, 4)
        for k in colours:
            accumulate(t, k, 0, 0, 3)
            accumulate(t, k, 0, 1, 5)

    for k in colours:
        p = [pos[a] for a in ORDER[k]]
        rows = pl.ds(PART * k, PART)
        grad = work[k, p[0], 4 * p[1] + p[2]] * (1.0 / 128.0)
        m_new = BETA_ONE * m_ref[rows, :] + (1.0 - BETA_ONE) * grad
        v_new = BETA_TWO * v_ref[rows, :] + (1.0 - BETA_TWO) * grad * grad
        m_hat = m_new / (1.0 - BETA_ONE ** ADAM_STEP)
        v_hat = v_new / (1.0 - BETA_TWO ** ADAM_STEP)
        m_out[rows, :] = m_new
        v_out[rows, :] = v_new
        w_out[rows, :] = w_ref[rows, :] - LEARN_RATE * m_hat / (jnp.sqrt(v_hat) + ADAM_EPS)
    for k in colours:
        p = [pos[a] for a in ORDER[k]]
        own = 16 * p[0] + 4 * p[1] + p[2]
        if k < 2:
            ag[k, core, own] = w_out[pl.ds(APART * k, APART), :].astype(BF16)
        else:
            vals = jnp.concatenate([w_out[pl.ds(120, 57), :], jnp.zeros((3, 128), F32)], axis=0)
            ag[k, core, own] = vals.astype(BF16)

    def block(t, k, shift, half=None):
        p = [pos[a] for a in ORDER[k]]
        q = ring(ORDER[k][t], shift)
        size = (16, 4, 1)[t]
        start = (16 * q, 16 * p[0] + 4 * q, 16 * p[0] + 4 * p[1] + q)[t]
        if t == 2:
            at = ag.at[k, core, start]
            if half is None:
                return at
            return at.at[pl.ds(32 * half, 32 - 4 * half)]
        if half is not None:
            size = size // 2
            start = start + size * half
        return ag.at[k, core, pl.ds(start, size)]

    GPARTS = ((0, None, 1), (0, None, -1), (-1, 0, 1), (1, 1, -1))

    def gather(t, k, part, came=0):
        shift, half, way = GPARTS[part]
        ref = block(t, k, shift - came, half)
        return pltpu.make_async_remote_copy(
            src_ref=ref, dst_ref=ref,
            send_sem=asend.at[t, k, part], recv_sem=arecv.at[t, k, part],
            device_id=neighbour(ORDER[k][t], way), device_id_type=MESH)

    def arrived(t, k, part):
        gather(t, k, part, came=GPARTS[part][2]).wait_recv()

    def share(k, shift):
        q = ring(ORDER[k][0], shift)
        ref = ag.at[k, core, pl.ds(16 * q, 16)]
        return pltpu.make_async_remote_copy(
            src_ref=ref, dst_ref=ref,
            send_sem=gsend.at[k, q], recv_sem=grecv.at[k, q],
            device_id=partner, device_id_type=MESH)

    def shared(k, shift):
        q = ring(ORDER[k][0], shift)
        ref = ag.at[k, 1 - core, pl.ds(16 * q, 16)]
        pltpu.make_async_remote_copy(
            src_ref=ref, dst_ref=ref,
            send_sem=gsend.at[k, q], recv_sem=grecv.at[k, q],
            device_id=partner, device_id_type=MESH).wait_recv()

    for t in (2, 1, 0):
        for k in colours:
            gather(t, k, 0).start()
            gather(t, k, 1).start()
            if t == 0:
                share(k, 0).start()
        for k in colours:
            arrived(t, k, 0)
            gather(t, k, 2).start()
            arrived(t, k, 1)
            gather(t, k, 3).start()
            if t == 0:
                share(k, -1).start()
                share(k, 1).start()
        for k in colours:
            arrived(t, k, 2)
            arrived(t, k, 3)
            if t == 0:
                share(k, 2).start()
    for shift in (0, -1, 1, 2):
        for k in colours:
            shared(k, shift)

    for k in colours:
        for shift in (0, -1, 1, 2):
            d2d(k, ring(ORDER[k][0], shift)).wait_send()
            share(k, shift).wait_send()
        for t in range(3):
            for part in range(6):
                rs(t, k, part).wait_send()
            for part in range(4):
                gather(t, k, part).wait_send()


def apply_kernel(ids, ag, act, emb_out, attn_out, in_out, ff_out, vd_out, vf_out, y_out,
                 flat, emb_v, attn_v, in_v, out_v, vd_v, vf_v, rows_v, sems):
    for k in range(3):
        for c in range(2):
            def unpack(i, k=k, c=c):
                q1, q2, q3 = lax.div(i, 16), lax.rem(lax.div(i, 4), 4), lax.rem(i, 4)
                row = SHARD * shard_of(k, q1, q2, q3, c) + APART * k
                size = APART if k < 2 else 57
                flat[pl.ds(row, size), :] = ag[k, c, i].astype(F32)[:size]
            loop(64, unpack, unroll=2)

    stage = (emb_v, attn_v, in_v, out_v)
    outs = (emb_out, attn_out, in_out, ff_out)
    copies = []
    for n in range(4):
        tiles, base, dst = TILES[n], BASE[n], stage[n]

        def pack(g, tiles=tiles, base=base, dst=dst):
            rows = pl.ds(pl.multiple_of(16 * g, 16), 16)
            for c in range(tiles):
                vals = flat[pl.ds(base + g * (16 * tiles) + c, 16, stride=tiles), :]
                dst[rows, 128 * c:128 * c + 128] = vals.astype(BF16)
        loop(GROUPS[n] // 2, pack, unroll=8 // tiles)
        copy = pltpu.make_async_copy(dst, outs[n], sems.at[n])
        copy.start()
        copies.append(copy)
    vd_v[...] = flat[pl.ds(BASE[4], 54), :].astype(BF16)
    vf_v[...] = flat[pl.ds(BASE[5], 24), :].astype(BF16)
    for n, (src, dst) in enumerate(((vd_v, vd_out), (vf_v, vf_out))):
        copy = pltpu.make_async_copy(src, dst, sems.at[4 + n])
        copy.start()
        copies.append(copy)

    def look(i):
        rows_v[pl.ds(2 * i, 2), :] = flat[pl.ds(2 * ids[i], 2), :]
    loop(256, look, unroll=8)
    def bias(row, count):
        flat_vals = flat[pl.ds(row, count), :].astype(BF16).astype(F32)
        return jnp.concatenate([flat_vals[i:i + 1] for i in range(count)], axis=1)
    emb = jnp.concatenate([rows_v[pl.ds(0, 256, stride=2), :], rows_v[pl.ds(1, 256, stride=2), :]], axis=1)
    hidden = (emb * 16.0 + act[...].astype(F32)).astype(BF16)
    pre = jnp.dot(hidden, in_v[0:256, :], preferred_element_type=F32) + bias(BASE[5], 8)
    inner = jax.nn.gelu(pre, approximate=True).astype(BF16)
    y = jnp.dot(inner, out_v[0:1024, :], preferred_element_type=F32) + bias(BASE[4] + 16, 2)
    y_out[...] = y.astype(BF16)
    for copy in copies:
        copy.wait()


def tiled(grad, width):
    flat = grad.reshape(-1, 8, width // 128, 128)
    return flat.transpose(0, 2, 1, 3)


def solution(mesh):
    def device_step(g_emb, g_attn, g_in, g_out, g_vecd, g_vecf, opt_m, opt_v, master, tok_ids, act_in):
        shapes = [g.shape[1:] for g in (g_emb, g_attn, g_in, g_out, g_vecd, g_vecf)]
        grads = (tiled(g_emb, 256), tiled(g_attn, 256), tiled(g_in, 1024), tiled(g_out, 256),
                 g_vecd.reshape(54, 128), g_vecf.reshape(24, 128))
        state = [s.reshape(SHARD, 128) for s in (opt_m, opt_v, master)]
        anywhere = pl.BlockSpec(memory_space=pltpu.HBM)
        vmem = pl.BlockSpec(memory_space=pltpu.VMEM)
        slots = pltpu.VMEM((3, 4, 16, PART, 128), F32)
        dma = pltpu.SemaphoreType.DMA
        shard = jax.ShapeDtypeStruct((SHARD, 128), F32)
        m_new, v_new, w_new, gathered = pl.pallas_call(
            sync_kernel,
            name="sync",
            out_shape=(shard, shard, shard, jax.ShapeDtypeStruct((3, 2, 64, APART, 128), BF16)),
            in_specs=[anywhere] * 6 + [vmem] * 3,
            out_specs=[vmem] * 4,
            scratch_shapes=[pltpu.VMEM(g.shape, F32) for g in grads] + [
                pltpu.VMEM((ROWS, 128), F32), slots, slots, slots,
                pltpu.VMEM((3, 6, 8, PART, 128), F32),
                pltpu.VMEM((3, 6, 2, PART, 128), F32),
                pltpu.VMEM((3, 6, 32, 128), F32),
                dma((6,)), dma((3, 4)), dma((3, 4)), dma((3, 3, 6)), dma((3, 3, 6)),
                dma((3, 3, 4)), dma((3, 3, 4)), dma((3, 4)), dma((3, 4))],
            compiler_params=pltpu.CompilerParams(
                collective_id=0, has_side_effects=True, vmem_limit_bytes=67043328),
        )(*grads, *state)

        flat_shapes = [(2048, 256), (3072, 256), (768, 1024), (3072, 256), (54, 128), (24, 128)]
        outs = pl.pallas_call(
            apply_kernel,
            name="apply",
            out_shape=[jax.ShapeDtypeStruct(s, BF16) for s in flat_shapes + [(256, 256)]],
            in_specs=[pl.BlockSpec(memory_space=pltpu.SMEM), vmem, vmem],
            out_specs=[anywhere] * 6 + [vmem],
            scratch_shapes=[pltpu.VMEM((ROWS, 128), F32)] + [pltpu.VMEM(s, BF16) for s in flat_shapes] + [
                pltpu.VMEM((512, 128), F32), dma((6,))],
            compiler_params=pltpu.CompilerParams(vmem_limit_bytes=67043328),
        )(tok_ids, gathered, act_in)
        halves = [o.reshape(s) for o, s in zip(outs[:6], shapes)]
        return (m_new.reshape(-1), v_new.reshape(-1), w_new.reshape(-1), *halves, outs[6])

    grad_specs = tuple(P(AXES, *([None] * (grad_rank - 1))) for grad_rank in GRAD_RANKS)
    in_specs = grad_specs + (P(AXES), P(AXES), P(AXES), P(AXES), P(AXES, None))
    out_specs = (P(AXES), P(AXES), P(AXES), P(), P(), P(), P(), P(), P(), P(AXES, None))
    return jax.shard_map(device_step, mesh=mesh, in_specs=in_specs, out_specs=out_specs, check_vma=False)
```

```python
import functools
import math
import jax
import jax.numpy as jnp
from jax import lax
from jax.experimental import pallas as pl
from jax.experimental.pallas import tpu as pltpu
from jax.sharding import PartitionSpec as P

LEARN_RATE = 0.002
BETA_ONE = 0.9
BETA_TWO = 0.95
ADAM_EPS = 1e-8
ADAM_STEP = 2
AXES = ("dz", "dy", "dx")
GRAD_RANKS = (3, 5, 4, 4, 4, 3)
MESH = pl.DeviceIdType.MESH

SHARD = 177
PART = 59
APART = 60
ROWS = 22656
REAL = 22606
BASE = (0, 4096, 10240, 16384, 22528, 22582)
GROUPS = (256, 384, 96, 384)
TILES = (2, 2, 8, 2)
ORDER = ((0, 1, 2), (1, 2, 0), (2, 0, 1))
F32 = jnp.float32
BF16 = jnp.bfloat16


def loop(count, body, unroll=1):
    def step(i, carry):
        body(i)
        return carry
    lax.fori_loop(0, count, step, 0, unroll=unroll)


def shard_of(k, q1, q2, q3, core):
    pos = [None] * 3
    for axis, q in zip(ORDER[k], (q1, q2, q3)):
        pos[axis] = q
    return pos[2] * 32 + pos[1] * 8 + pos[0] * 2 + core


def sync_kernel(e_hbm, a_hbm, i_hbm, o_hbm, vd_hbm, vf_hbm, m_ref, v_ref, w_ref,
                m_out, v_out, w_out, flat,
                e_raw, a_raw, i_raw, o_raw, vd_raw, vf_raw, ag, psl, work, drx,
                r1, r2, r3,
                raw_sem, dsend, drecv, ssend, srecv, asend, arecv, gsend, grecv):
    dz, dy, dx = lax.axis_index("dz"), lax.axis_index("dy"), lax.axis_index("dx")
    core = lax.rem(dx, 2)
    pos = (lax.div(dx, 2), dy, dz)
    partner = {"dz": dz, "dy": dy, "dx": dx + 1 - 2 * core}

    def neighbour(axis, shift):
        q = lax.rem(pos[axis] + 4 + shift, 4)
        if axis == 0:
            return {"dz": dz, "dy": dy, "dx": q * 2 + core}
        if axis == 1:
            return {"dz": dz, "dy": q, "dx": dx}
        return {"dz": q, "dy": dy, "dx": dx}

    def ring(axis, shift):
        return lax.rem(pos[axis] + 4 + shift, 4)

    barrier = pltpu.get_barrier_semaphore()
    for axis in range(3):
        for shift in (1, -1):
            pl.semaphore_signal(barrier, inc=1, device_id=neighbour(axis, shift), device_id_type=MESH)
    pl.semaphore_signal(barrier, inc=1, device_id=partner, device_id_type=MESH)

    raws = (e_raw, a_raw, i_raw, o_raw, vd_raw, vf_raw)
    loads = [pltpu.make_async_copy(src, dst, raw_sem.at[n]) for n, (src, dst) in enumerate(
        zip((e_hbm, a_hbm, i_hbm, o_hbm, vd_hbm, vf_hbm), raws))]
    for n in (0, 1, 2, 3, 4, 5):
        loads[n].start()

    flat[pl.ds(REAL, ROWS - REAL), :] = jnp.zeros((ROWS - REAL, 128), F32)
    for n in range(4):
        loads[n].wait()
        tiles, base, raw = TILES[n], BASE[n], raws[n]

        def relayout(g, tiles=tiles, base=base, raw=raw):
            for c in range(tiles):
                flat[pl.ds(base + g * (8 * tiles) + c, 8, stride=tiles), :] = raw[g, c]
        loop(GROUPS[n], relayout, unroll=16 // tiles)
    loads[4].wait()
    for i in range(27):
        for h in range(2):
            flat[pl.ds(BASE[4] + 2 * i + h, 1), :] = vd_raw[i, :, 128 * h:128 * h + 128]
    loads[5].wait()
    flat[pl.ds(BASE[5], 24), :] = vf_raw[...]

    pl.semaphore_wait(barrier, 7)

    def flat_row(k, q1, j, c):
        return SHARD * shard_of(k, q1, lax.div(j, 4), lax.rem(j, 4), c) + PART * k

    def d2d(k, q1):
        return pltpu.make_async_remote_copy(
            src_ref=psl.at[k, q1], dst_ref=drx.at[k, q1],
            send_sem=dsend.at[k, q1], recv_sem=drecv.at[k, q1],
            device_id=partner, device_id_type=MESH)

    for shift in (2, 1, -1, 0):
        for k in range(3):
            q1 = ring(ORDER[k][0], shift)

            def pick(j, k=k, q1=q1):
                psl[k, q1, j] = flat[pl.ds(flat_row(k, q1, j, 1 - core), PART), :]
            loop(16, pick, unroll=2)
            d2d(k, q1).start()

    def add_core(k, shift):
        q1 = ring(ORDER[k][0], shift)
        d2d(k, q1).wait_recv()

        def body(j):
            work[k, q1, j] = flat[pl.ds(flat_row(k, q1, j, core), PART), :] + drx[k, q1, j]
        loop(16, body, unroll=2)

    def chunk(t, k, shift, half):
        p = [pos[a] for a in ORDER[k]]
        q = ring(ORDER[k][t], shift)
        if t == 0:
            return work.at[k, q, pl.ds(8 * half, 8)]
        if t == 1:
            return work.at[k, p[0], pl.ds(4 * q + 2 * half, 2)]
        return work.at[k, p[0], 4 * p[1] + q, pl.ds(32 * half, 32 - 5 * half)]

    def landing(t, k, part, half):
        if t == 0:
            return r1.at[k, part]
        if t == 1:
            return r2.at[k, part]
        return r3.at[k, part, pl.ds(0, 32 - 5 * half)]

    PARTS = ((2, 0, 1), (2, 1, -1), (1, 1, 1), (1, 0, 1), (-1, 0, -1), (-1, 1, -1))

    def rs(t, k, part):
        shift, half, way = PARTS[part]
        return pltpu.make_async_remote_copy(
            src_ref=chunk(t, k, shift, half), dst_ref=landing(t, k, part, half),
            send_sem=ssend.at[t, k, part], recv_sem=srecv.at[t, k, part],
            device_id=neighbour(ORDER[k][t], way), device_id_type=MESH)

    def accumulate(t, k, shift, half, part):
        rs(t, k, part).wait_recv()
        dst = chunk(t, k, shift, half)
        src = landing(t, k, part, half)
        if t == 0:
            def body(j):
                dst[j] = dst[j] + src[j]
            loop(8, body, unroll=2)
        else:
            dst[...] = dst[...] + src[...]

    colours = range(3)
    for t in range(3):
        if t == 0:
            for k in colours:
                add_core(k, 2)
                rs(t, k, 0).start()
                rs(t, k, 1).start()
            for k in colours:
                add_core(k, 1)
                rs(t, k, 2).start()
                add_core(k, -1)
                rs(t, k, 4).start()
        else:
            for k in colours:
                rs(t, k, 0).start()
                rs(t, k, 1).start()
                rs(t, k, 2).start()
                rs(t, k, 4).start()
        for k in colours:
            accumulate(t, k, 1, 0, 0)
            rs(t, k, 3).start()
            accumulate(t, k, -1, 1, 1)
            rs(t, k, 5).start()
        if t == 0:
            for k in colours:
                add_core(k, 0)
        for k in colours:
            accumulate(t, k, 0, 1, 2)
            accumulate(t, k, 0, 0, 4)
        for k in colours:
            accumulate(t, k, 0, 0, 3)
            accumulate(t, k, 0, 1, 5)

    for k in colours:
        p = [pos[a] for a in ORDER[k]]
        rows = pl.ds(PART * k, PART)
        grad = work[k, p[0], 4 * p[1] + p[2]] * (1.0 / 128.0)
        m_new = BETA_ONE * m_ref[rows, :] + (1.0 - BETA_ONE) * grad
        v_new = BETA_TWO * v_ref[rows, :] + (1.0 - BETA_TWO) * grad * grad
        m_hat = m_new / (1.0 - BETA_ONE ** ADAM_STEP)
        v_hat = v_new / (1.0 - BETA_TWO ** ADAM_STEP)
        m_out[rows, :] = m_new
        v_out[rows, :] = v_new
        w_out[rows, :] = w_ref[rows, :] - LEARN_RATE * m_hat / (jnp.sqrt(v_hat) + ADAM_EPS)
    for k in colours:
        p = [pos[a] for a in ORDER[k]]
        own = 16 * p[0] + 4 * p[1] + p[2]
        if k < 2:
            ag[k, core, own] = w_out[pl.ds(APART * k, APART), :].astype(BF16)
        else:
            vals = jnp.concatenate([w_out[pl.ds(120, 57), :], jnp.zeros((3, 128), F32)], axis=0)
            ag[k, core, own] = vals.astype(BF16)

    def block(t, k, shift, half=None):
        p = [pos[a] for a in ORDER[k]]
        q = ring(ORDER[k][t], shift)
        size = (16, 4, 1)[t]
        start = (16 * q, 16 * p[0] + 4 * q, 16 * p[0] + 4 * p[1] + q)[t]
        if t == 2:
            at = ag.at[k, core, start]
            if half is None:
                return at
            return at.at[pl.ds(32 * half, 32 - 4 * half)]
        if half is not None:
            size = size // 2
            start = start + size * half
        return ag.at[k, core, pl.ds(start, size)]

    GPARTS = ((0, None, 1), (0, None, -1), (-1, 0, 1), (1, 1, -1))

    def gather(t, k, part, came=0):
        shift, half, way = GPARTS[part]
        ref = block(t, k, shift - came, half)
        return pltpu.make_async_remote_copy(
            src_ref=ref, dst_ref=ref,
            send_sem=asend.at[t, k, part], recv_sem=arecv.at[t, k, part],
            device_id=neighbour(ORDER[k][t], way), device_id_type=MESH)

    def arrived(t, k, part):
        gather(t, k, part, came=GPARTS[part][2]).wait_recv()

    def share(k, shift):
        q = ring(ORDER[k][0], shift)
        ref = ag.at[k, core, pl.ds(16 * q, 16)]
        return pltpu.make_async_remote_copy(
            src_ref=ref, dst_ref=ref,
            send_sem=gsend.at[k, q], recv_sem=grecv.at[k, q],
            device_id=partner, device_id_type=MESH)

    def shared(k, shift):
        q = ring(ORDER[k][0], shift)
        ref = ag.at[k, 1 - core, pl.ds(16 * q, 16)]
        pltpu.make_async_remote_copy(
            src_ref=ref, dst_ref=ref,
            send_sem=gsend.at[k, q], recv_sem=grecv.at[k, q],
            device_id=partner, device_id_type=MESH).wait_recv()

    def unpack(k, c, shift):
        q1 = ring(ORDER[k][0], shift)
        size = APART if k < 2 else 57

        def body(j):
            row = SHARD * shard_of(k, q1, lax.div(j, 4), lax.rem(j, 4), c) + APART * k
            flat[pl.ds(row, size), :] = ag[k, c, 16 * q1 + j].astype(F32)[:size]
        loop(16, body, unroll=2)

    for t in (2, 1, 0):
        for k in colours:
            gather(t, k, 0).start()
            gather(t, k, 1).start()
            if t == 0:
                share(k, 0).start()
        if t == 0:
            for k in colours:
                unpack(k, core, 0)
        for k in colours:
            arrived(t, k, 0)
            gather(t, k, 2).start()
            arrived(t, k, 1)
            gather(t, k, 3).start()
            if t == 0:
                share(k, -1).start()
                share(k, 1).start()
        for k in colours:
            arrived(t, k, 2)
            arrived(t, k, 3)
            if t == 0:
                share(k, 2).start()
    for shift in (-1, 1, 2):
        for k in colours:
            unpack(k, core, shift)
    for shift in (0, -1, 1, 2):
        for k in colours:
            shared(k, shift)
            unpack(k, 1 - core, shift)

    for k in colours:
        for shift in (0, -1, 1, 2):
            d2d(k, ring(ORDER[k][0], shift)).wait_send()
            share(k, shift).wait_send()
        for t in range(3):
            for part in range(6):
                rs(t, k, part).wait_send()
            for part in range(4):
                gather(t, k, part).wait_send()


def apply_kernel(ids, flat, act, m_in, v_in, w_in,
                 emb_out, attn_out, in_out, ff_out, vd_out, vf_out, y_out, m_out, v_out, w_out,
                 emb_v, attn_v, in_v, out_v, vd_v, vf_v, rows_v, sems):
    copies = []

    def send(src, dst):
        copy = pltpu.make_async_copy(src, dst, sems.at[len(copies)])
        copy.start()
        copies.append(copy)

    for src, dst in ((m_in, m_out), (v_in, v_out), (w_in, w_out)):
        send(src, dst)
    stage = (emb_v, attn_v, in_v, out_v)
    outs = (emb_out, attn_out, in_out, ff_out)
    for n in range(4):
        tiles, base, dst = TILES[n], BASE[n], stage[n]

        def pack(g, tiles=tiles, base=base, dst=dst):
            rows = pl.ds(pl.multiple_of(16 * g, 16), 16)
            for c in range(tiles):
                vals = flat[pl.ds(base + g * (16 * tiles) + c, 16, stride=tiles), :]
                dst[rows, 128 * c:128 * c + 128] = vals.astype(BF16)
        loop(GROUPS[n] // 2, pack, unroll=8 // tiles)
        send(dst, outs[n])
    for r in range(9):
        for h in range(2):
            vals = flat[pl.ds(BASE[4] + 2 * r + h, 3, stride=18), :]
            vd_v[r, :, 128 * h:128 * h + 128] = vals.astype(BF16)
    for c in range(8):
        vf_v[:, 128 * c:128 * c + 128] = flat[pl.ds(BASE[5] + c, 3, stride=8), :].astype(BF16)
    send(vd_v, vd_out)
    send(vf_v, vf_out)

    def look(i):
        rows_v[pl.ds(2 * i, 2), :] = flat[pl.ds(2 * ids[i], 2), :]
    loop(256, look, unroll=8)

    def bias(row, count):
        flat_vals = flat[pl.ds(row, count), :].astype(BF16).astype(F32)
        return jnp.concatenate([flat_vals[i:i + 1] for i in range(count)], axis=1)
    emb = jnp.concatenate([rows_v[pl.ds(0, 256, stride=2), :], rows_v[pl.ds(1, 256, stride=2), :]], axis=1)
    hidden = (emb * 16.0 + act[...].astype(F32)).astype(BF16)
    pre = jnp.dot(hidden, in_v[0:256, :], preferred_element_type=F32) + bias(BASE[5], 8)
    inner = jax.nn.gelu(pre, approximate=True).astype(BF16)
    y = jnp.dot(inner, out_v[0:1024, :], preferred_element_type=F32) + bias(BASE[4] + 16, 2)
    y_out[...] = y.astype(BF16)
    for copy in copies:
        copy.wait()


def tiled(grad, width):
    flat = grad.reshape(-1, 8, width // 128, 128)
    return flat.transpose(0, 2, 1, 3)


def solution(mesh):
    def device_step(g_emb, g_attn, g_in, g_out, g_vecd, g_vecf, opt_m, opt_v, master, tok_ids, act_in):
        shapes = [g.shape[1:] for g in (g_emb, g_attn, g_in, g_out, g_vecd, g_vecf)]
        grads = (tiled(g_emb, 256), tiled(g_attn, 256), tiled(g_in, 1024), tiled(g_out, 256),
                 g_vecd.transpose(1, 2, 0, 3).reshape(27, 1, 256), g_vecf.reshape(24, 128))
        state = [s.reshape(SHARD, 128) for s in (opt_m, opt_v, master)]
        anywhere = pl.BlockSpec(memory_space=pltpu.HBM)
        vmem = pl.BlockSpec(memory_space=pltpu.VMEM)
        slots = pltpu.VMEM((3, 4, 16, PART, 128), F32)
        dma = pltpu.SemaphoreType.DMA
        shard = pltpu.VMEM((SHARD, 128), F32)
        m_new, v_new, w_new, flat = pl.pallas_call(
            sync_kernel,
            name="sync",
            out_shape=(shard, shard, shard, pltpu.VMEM((ROWS, 128), F32)),
            in_specs=[anywhere] * 6 + [vmem] * 3,
            out_specs=[vmem] * 4,
            scratch_shapes=[pltpu.VMEM(g.shape, F32) for g in grads] + [
                pltpu.VMEM((3, 2, 64, APART, 128), BF16), slots, slots, slots,
                pltpu.VMEM((3, 6, 8, PART, 128), F32),
                pltpu.VMEM((3, 6, 2, PART, 128), F32),
                pltpu.VMEM((3, 6, 32, 128), F32),
                dma((6,)), dma((3, 4)), dma((3, 4)), dma((3, 3, 6)), dma((3, 3, 6)),
                dma((3, 3, 4)), dma((3, 3, 4)), dma((3, 4)), dma((3, 4))],
            compiler_params=pltpu.CompilerParams(
                collective_id=0, has_side_effects=True, vmem_limit_bytes=50 * 1048576),
        )(*grads, *state)

        staged = [(2048, 256), (3072, 256), (768, 1024), (3072, 256), (9, 3, 256), (3, 1024)]
        state_out = jax.ShapeDtypeStruct((SHARD, 128), F32)
        outs = pl.pallas_call(
            apply_kernel,
            name="apply",
            out_shape=[jax.ShapeDtypeStruct(s, BF16) for s in staged + [(256, 256)]] + [state_out] * 3,
            in_specs=[pl.BlockSpec(memory_space=pltpu.SMEM)] + [vmem] * 5,
            out_specs=[anywhere] * 6 + [vmem] + [anywhere] * 3,
            scratch_shapes=[pltpu.VMEM(s, BF16) for s in staged] + [
                pltpu.VMEM((512, 128), F32), dma((9,))],
            compiler_params=pltpu.CompilerParams(vmem_limit_bytes=24 * 1048576),
        )(tok_ids, flat, act_in, m_new, v_new, w_new)
        halves = [o.reshape(s) for o, s in zip(outs[:4], shapes)]
        halves += [outs[4].transpose(1, 0, 2), outs[5]]
        return (*[o.reshape(-1) for o in outs[7:]], *halves, outs[6])

    grad_specs = tuple(P(AXES, *([None] * (grad_rank - 1))) for grad_rank in GRAD_RANKS)
    in_specs = grad_specs + (P(AXES), P(AXES), P(AXES), P(AXES), P(AXES, None))
    out_specs = (P(AXES), P(AXES), P(AXES), P(), P(), P(), P(), P(), P(), P(AXES, None))
    return jax.shard_map(device_step, mesh=mesh, in_specs=in_specs, out_specs=out_specs, check_vma=False)
```

```python
import functools
import math
import jax
import jax.numpy as jnp
from jax import lax
from jax.experimental import pallas as pl
from jax.experimental.pallas import tpu as pltpu
from jax.sharding import PartitionSpec as P

LEARN_RATE = 0.002
BETA_ONE = 0.9
BETA_TWO = 0.95
ADAM_EPS = 1e-8
ADAM_STEP = 2
AXES = ("dz", "dy", "dx")
GRAD_RANKS = (3, 5, 4, 4, 4, 3)
MESH = pl.DeviceIdType.MESH

SHARD = 177
PART = 59
APART = 60
ROWS = 22656
REAL = 22606
BASE = (0, 4096, 10240, 16384, 22528, 22582)
GROUPS = (256, 384, 96, 384)
TILES = (2, 2, 8, 2)
ORDER = ((0, 1, 2), (1, 2, 0), (2, 0, 1))
F32 = jnp.float32
BF16 = jnp.bfloat16


def loop(count, body, unroll=1):
    def step(i, carry):
        body(i)
        return carry
    lax.fori_loop(0, count, step, 0, unroll=unroll)


def shard_of(k, q1, q2, q3, core):
    pos = [None] * 3
    for axis, q in zip(ORDER[k], (q1, q2, q3)):
        pos[axis] = q
    return pos[2] * 32 + pos[1] * 8 + pos[0] * 2 + core


def sync_kernel(e_hbm, a_hbm, i_hbm, o_hbm, vd_hbm, vf_hbm, m_ref, v_ref, w_ref,
                m_out, v_out, w_out, flat,
                e_raw, a_raw, i_raw, o_raw, vd_raw, vf_raw, ag, psl, work, drx,
                r1, r2, r3,
                raw_sem, dsend, drecv, s1send, s1recv, s2send, s2recv, s3send, s3recv,
                g2send, g2recv, g1send, g1recv, g0send, g0recv, shsend, shrecv):
    dz, dy, dx = lax.axis_index("dz"), lax.axis_index("dy"), lax.axis_index("dx")
    core = lax.rem(dx, 2)
    pos = (lax.div(dx, 2), dy, dz)
    partner = {"dz": dz, "dy": dy, "dx": dx + 1 - 2 * core}
    colours = range(3)
    FAR = (2, 1, -1, 0)

    def neighbour(axis, shift):
        q = lax.rem(pos[axis] + 4 + shift, 4)
        if axis == 0:
            return {"dz": dz, "dy": dy, "dx": q * 2 + core}
        if axis == 1:
            return {"dz": dz, "dy": q, "dx": dx}
        return {"dz": q, "dy": dy, "dx": dx}

    def ring(axis, shift):
        return lax.rem(pos[axis] + 4 + shift, 4)

    def remote(src, dst, send_sem, recv_sem, device):
        return pltpu.make_async_remote_copy(
            src_ref=src, dst_ref=dst, send_sem=send_sem, recv_sem=recv_sem,
            device_id=device, device_id_type=MESH)

    barrier = pltpu.get_barrier_semaphore()
    for axis in range(3):
        for shift in (1, -1, 2):
            pl.semaphore_signal(barrier, inc=1, device_id=neighbour(axis, shift), device_id_type=MESH)
    pl.semaphore_signal(barrier, inc=1, device_id=partner, device_id_type=MESH)

    raws = (e_raw, a_raw, i_raw, o_raw, vd_raw, vf_raw)
    loads = [pltpu.make_async_copy(src, dst, raw_sem.at[n]) for n, (src, dst) in enumerate(
        zip((e_hbm, a_hbm, i_hbm, o_hbm, vd_hbm, vf_hbm), raws))]
    for n in (0, 1, 2, 3, 4, 5):
        loads[n].start()

    flat[pl.ds(REAL, ROWS - REAL), :] = jnp.zeros((ROWS - REAL, 128), F32)
    for n in range(4):
        with jax.named_scope(f"load{n}"):
            loads[n].wait()
        tiles, base, raw = TILES[n], BASE[n], raws[n]

        def relayout(g, tiles=tiles, base=base, raw=raw):
            for c in range(tiles):
                flat[pl.ds(base + g * (8 * tiles) + c, 8, stride=tiles), :] = raw[g, c]
        loop(GROUPS[n], relayout, unroll=16 // tiles)
    loads[4].wait()
    for i in range(27):
        for h in range(2):
            flat[pl.ds(BASE[4] + 2 * i + h, 1), :] = vd_raw[i, :, 128 * h:128 * h + 128]
    loads[5].wait()
    flat[pl.ds(BASE[5], 24), :] = vf_raw[...]

    with jax.named_scope("enter"):
        pl.semaphore_wait(barrier, 10)

    def d2d(k, i1, i2):
        q1, q2 = ring(ORDER[k][0], FAR[i1]), ring(ORDER[k][1], FAR[i2])
        at = (k, q1, pl.ds(4 * q2, 4))
        return remote(psl.at[at], drx.at[at], dsend.at[k, i1, i2], drecv.at[k, i1, i2], partner)

    for i2 in range(4):
        for i1 in range(4):
            for k in colours:
                q1, q2 = ring(ORDER[k][0], FAR[i1]), ring(ORDER[k][1], FAR[i2])

                def pick(j, k=k, q1=q1, q2=q2):
                    row = SHARD * shard_of(k, q1, q2, j, 1 - core) + PART * k
                    psl[k, q1, 4 * q2 + j] = flat[pl.ds(row, PART), :]
                loop(4, pick, unroll=2)
                d2d(k, i1, i2).start()

    def add_core(k, i1, i2):
        q1, q2 = ring(ORDER[k][0], FAR[i1]), ring(ORDER[k][1], FAR[i2])
        with jax.named_scope(f"d2d{i2}_{i1}_{k}"):
            d2d(k, i1, i2).wait_recv()

        def body(j):
            row = SHARD * shard_of(k, q1, q2, j, core) + PART * k
            work[k, q1, 4 * q2 + j] = flat[pl.ds(row, PART), :] + drx[k, q1, 4 * q2 + j]
        loop(4, body, unroll=2)

    PARTS = ((2, 0, 1), (2, 1, -1), (1, 1, 1), (1, 0, 1), (-1, 0, -1), (-1, 1, -1))

    def chunk1(k, i2, shift, half):
        q1, q2 = ring(ORDER[k][0], shift), ring(ORDER[k][1], FAR[i2])
        return work.at[k, q1, pl.ds(4 * q2 + 2 * half, 2)]

    def chunk2(k, shift, half):
        q1, q2 = ring(ORDER[k][0], 0), ring(ORDER[k][1], shift)
        return work.at[k, q1, pl.ds(4 * q2 + 2 * half, 2)]

    def own3(k, shift):
        q1, q2, q3 = ring(ORDER[k][0], 0), ring(ORDER[k][1], 0), ring(ORDER[k][2], shift)
        return work.at[k, q1, 4 * q2 + q3]

    def rs1(k, i2, part):
        shift, half, way = PARTS[part]
        return remote(chunk1(k, i2, shift, half), r1.at[k, i2, part],
                      s1send.at[k, i2, part], s1recv.at[k, i2, part], neighbour(ORDER[k][0], way))

    def rs2(k, part):
        shift, half, way = PARTS[part]
        return remote(chunk2(k, shift, half), r2.at[k, part],
                      s2send.at[k, part], s2recv.at[k, part], neighbour(ORDER[k][1], way))

    def rs3(k, i3):
        return remote(own3(k, FAR[i3]), r3.at[k, i3],
                      s3send.at[k, i3], s3recv.at[k, i3], neighbour(ORDER[k][2], FAR[i3]))

    def add1(k, i2, shift, half, part):
        with jax.named_scope(f"a{i2}_{part}_{k}"):
            rs1(k, i2, part).wait_recv()
        dst = chunk1(k, i2, shift, half)
        dst[...] = dst[...] + r1[k, i2, part]

    def add2(k, shift, half, part):
        with jax.named_scope(f"b{part}_{k}"):
            rs2(k, part).wait_recv()
        dst = chunk2(k, shift, half)
        dst[...] = dst[...] + r2[k, part]

    def first(i2):
        for k in colours:
            add_core(k, 0, i2)
            rs1(k, i2, 0).start()
            rs1(k, i2, 1).start()
        for k in colours:
            add_core(k, 1, i2)
            rs1(k, i2, 2).start()
            add_core(k, 2, i2)
            rs1(k, i2, 4).start()

    def relay(i2):
        for k in colours:
            add1(k, i2, 1, 0, 0)
            rs1(k, i2, 3).start()
            add1(k, i2, -1, 1, 1)
            rs1(k, i2, 5).start()

    def finish(i2):
        for k in colours:
            add_core(k, 3, i2)
            add1(k, i2, 0, 1, 2)
            add1(k, i2, 0, 0, 4)
            add1(k, i2, 0, 0, 3)
            add1(k, i2, 0, 1, 5)
            if i2 == 0:
                rs2(k, 0).start()
                rs2(k, 1).start()
            if i2 == 1:
                rs2(k, 2).start()
            if i2 == 2:
                rs2(k, 4).start()

    first(0)
    first(1)
    relay(0)
    first(2)
    relay(1)
    finish(0)
    first(3)
    relay(2)
    finish(1)
    relay(3)
    finish(2)
    for k in colours:
        add2(k, 1, 0, 0)
        rs2(k, 3).start()
        add2(k, -1, 1, 1)
        rs2(k, 5).start()
    finish(3)
    for k in colours:
        add2(k, 0, 1, 2)
        add2(k, 0, 0, 4)
        add2(k, 0, 0, 3)
        add2(k, 0, 1, 5)
        for i3 in range(3):
            rs3(k, i3).start()

    for k in colours:
        rows = pl.ds(PART * k, PART)
        grad = own3(k, 0)[...]
        for i3 in range(3):
            with jax.named_scope(f"c{i3}_{k}"):
                rs3(k, i3).wait_recv()
            grad = grad + r3[k, i3]
        grad = grad * (1.0 / 128.0)
        m_new = BETA_ONE * m_ref[rows, :] + (1.0 - BETA_ONE) * grad
        v_new = BETA_TWO * v_ref[rows, :] + (1.0 - BETA_TWO) * grad * grad
        m_hat = m_new / (1.0 - BETA_ONE ** ADAM_STEP)
        v_hat = v_new / (1.0 - BETA_TWO ** ADAM_STEP)
        m_out[rows, :] = m_new
        v_out[rows, :] = v_new
        w_out[rows, :] = w_ref[rows, :] - LEARN_RATE * m_hat / (jnp.sqrt(v_hat) + ADAM_EPS)

    def slot(k, s1, s2, s3):
        axes = ORDER[k]
        return 16 * ring(axes[0], s1) + 4 * ring(axes[1], s2) + ring(axes[2], s3)

    for k in colours:
        own = slot(k, 0, 0, 0)
        if k < 2:
            ag[k, core, own] = w_out[pl.ds(APART * k, APART), :].astype(BF16)
        else:
            vals = jnp.concatenate([w_out[pl.ds(120, 57), :], jnp.zeros((3, 128), F32)], axis=0)
            ag[k, core, own] = vals.astype(BF16)

    def unpack(k, c, s1, s2):
        q1, q2 = ring(ORDER[k][0], s1), ring(ORDER[k][1], s2)
        size = APART if k < 2 else 57

        def body(j):
            row = SHARD * shard_of(k, q1, q2, j, c) + APART * k
            flat[pl.ds(row, size), :] = ag[k, c, 16 * q1 + 4 * q2 + j].astype(F32)[:size]
        loop(4, body, unroll=2)

    NEAR = (0, -1, 1, 2)

    def g2(k, i, came):
        way = (1, -1, 2)[i]
        ref = ag.at[k, core, slot(k, 0, 0, -way if came else 0)]
        return remote(ref, ref, g2send.at[k, i], g2recv.at[k, i], neighbour(ORDER[k][2], way))

    def g1(k, i3, part, came):
        onward = 1 if i3 in (0, 3) else -1
        way = (1, -1, onward)[part]
        start = (0, 0, -onward)[part]
        ref = ag.at[k, core, slot(k, 0, start - way if came else start, NEAR[i3])]
        return remote(ref, ref, g1send.at[k, i3, part], g1recv.at[k, i3, part], neighbour(ORDER[k][1], way))

    def g0(k, i2, part, came):
        way = (1, -1, 1, -1)[part]
        start = (0, 0, -1, 1)[part]
        q1 = ring(ORDER[k][0], start - way if came else start)
        at = 16 * q1 + 4 * ring(ORDER[k][1], NEAR[i2])
        if part >= 2:
            ref = ag.at[k, core, pl.ds(at + 2 * (part - 2), 2)]
        else:
            ref = ag.at[k, core, pl.ds(at, 4)]
        return remote(ref, ref, g0send.at[k, i2, part], g0recv.at[k, i2, part], neighbour(ORDER[k][0], way))

    def share(k, i1, i2, c):
        at = 16 * ring(ORDER[k][0], NEAR[i1]) + 4 * ring(ORDER[k][1], NEAR[i2])
        ref = ag.at[k, c, pl.ds(at, 4)]
        return remote(ref, ref, shsend.at[k, i1, i2], shrecv.at[k, i1, i2], partner)

    def give(k, i1, i2):
        share(k, i1, i2, core).start()

    def take(k, i1, i2):
        with jax.named_scope(f"s{i1}_{i2}_{k}"):
            share(k, i1, i2, 1 - core).wait_recv()
        unpack(k, 1 - core, NEAR[i1], NEAR[i2])

    def got(copy, name):
        with jax.named_scope(name):
            copy.wait_recv()

    def group(k, i2):
        g0(k, i2, 0, False).start()
        g0(k, i2, 1, False).start()
        give(k, 0, i2)

    def onward0(k, i2):
        got(g0(k, i2, 0, True), f"f{i2}_0_{k}")
        g0(k, i2, 2, False).start()
        give(k, 1, i2)
        got(g0(k, i2, 1, True), f"f{i2}_1_{k}")
        g0(k, i2, 3, False).start()
        give(k, 2, i2)

    def last0(k, i2):
        got(g0(k, i2, 2, True), f"f{i2}_2_{k}")
        got(g0(k, i2, 3, True), f"f{i2}_3_{k}")
        give(k, 3, i2)

    for k in colours:
        for i in range(3):
            g2(k, i, False).start()
        g1(k, 0, 0, False).start()
        g1(k, 0, 1, False).start()
    for i in range(3):
        for k in colours:
            got(g2(k, i, True), f"d{i}_{k}")
            g1(k, i + 1, 0, False).start()
            g1(k, i + 1, 1, False).start()
            if i == 2:
                group(k, 0)
    for k in colours:
        unpack(k, core, 0, 0)
    for i3 in range(4):
        for k in colours:
            for part in range(2):
                got(g1(k, i3, part, True), f"e{i3}_{part}_{k}")
                if part == (0 if i3 in (0, 3) else 1):
                    g1(k, i3, 2, False).start()
            if i3 == 3:
                group(k, 1)
                group(k, 2)
    for k in colours:
        onward0(k, 0)
    for k in colours:
        for i3 in range(4):
            got(g1(k, i3, 2, True), f"e{i3}_2_{k}")
        group(k, 3)
    for k in colours:
        for i2 in (1, 2, 3):
            unpack(k, core, 0, NEAR[i2])
    for k in colours:
        take(k, 0, 0)
    for k in colours:
        last0(k, 0)
    for i2 in (1, 2, 3):
        for k in colours:
            onward0(k, i2)
        for k in colours:
            for i1 in (1, 2):
                unpack(k, core, NEAR[i1], NEAR[i2 - 1])
                take(k, i1, i2 - 1)
            take(k, 0, i2)
            unpack(k, core, 2, NEAR[i2 - 1])
            take(k, 3, i2 - 1)
        for k in colours:
            last0(k, i2)
    for k in colours:
        for i1 in (1, 2, 3):
            unpack(k, core, NEAR[i1], NEAR[3])
    for i1 in (1, 2, 3):
        for k in colours:
            take(k, i1, 3)

    for k in colours:
        for i in range(4):
            for j in range(4):
                d2d(k, i, j).wait_send()
                share(k, i, j, core).wait_send()
                g0(k, i, j, False).wait_send()
            for part in range(6):
                rs1(k, i, part).wait_send()
            for part in range(3):
                g1(k, i, part, False).wait_send()
        for part in range(6):
            rs2(k, part).wait_send()
        for part in range(3):
            rs3(k, part).wait_send()
            g2(k, part, False).wait_send()


def apply_kernel(ids, flat, act, m_in, v_in, w_in,
                 emb_out, attn_out, in_out, ff_out, vd_out, vf_out, y_out, m_out, v_out, w_out,
                 emb_v, attn_v, in_v, out_v, vd_v, vf_v, rows_v, sems):
    copies = []

    def send(src, dst):
        copy = pltpu.make_async_copy(src, dst, sems.at[len(copies)])
        copy.start()
        copies.append(copy)

    for src, dst in ((m_in, m_out), (v_in, v_out), (w_in, w_out)):
        send(src, dst)
    stage = (emb_v, attn_v, in_v, out_v)
    outs = (emb_out, attn_out, in_out, ff_out)
    for n in range(4):
        tiles, base, dst = TILES[n], BASE[n], stage[n]

        def pack(g, tiles=tiles, base=base, dst=dst):
            rows = pl.ds(pl.multiple_of(16 * g, 16), 16)
            for c in range(tiles):
                vals = flat[pl.ds(base + g * (16 * tiles) + c, 16, stride=tiles), :]
                dst[rows, 128 * c:128 * c + 128] = vals.astype(BF16)
        loop(GROUPS[n] // 2, pack, unroll=8 // tiles)
        send(dst, outs[n])
    for r in range(9):
        for h in range(2):
            vals = flat[pl.ds(BASE[4] + 2 * r + h, 3, stride=18), :]
            vd_v[r, :, 128 * h:128 * h + 128] = vals.astype(BF16)
    for c in range(8):
        vf_v[:, 128 * c:128 * c + 128] = flat[pl.ds(BASE[5] + c, 3, stride=8), :].astype(BF16)
    send(vd_v, vd_out)
    send(vf_v, vf_out)

    def look(i):
        rows_v[pl.ds(2 * i, 2), :] = flat[pl.ds(2 * ids[i], 2), :]
    loop(256, look, unroll=8)

    def bias(row, count):
        flat_vals = flat[pl.ds(row, count), :].astype(BF16).astype(F32)
        return jnp.concatenate([flat_vals[i:i + 1] for i in range(count)], axis=1)
    emb = jnp.concatenate([rows_v[pl.ds(0, 256, stride=2), :], rows_v[pl.ds(1, 256, stride=2), :]], axis=1)
    hidden = (emb * 16.0 + act[...].astype(F32)).astype(BF16)
    pre = jnp.dot(hidden, in_v[0:256, :], preferred_element_type=F32) + bias(BASE[5], 8)
    inner = jax.nn.gelu(pre, approximate=True).astype(BF16)
    y = jnp.dot(inner, out_v[0:1024, :], preferred_element_type=F32) + bias(BASE[4] + 16, 2)
    y_out[...] = y.astype(BF16)
    for copy in copies:
        copy.wait()


def tiled(grad, width):
    flat = grad.reshape(-1, 8, width // 128, 128)
    return flat.transpose(0, 2, 1, 3)


def solution(mesh):
    def device_step(g_emb, g_attn, g_in, g_out, g_vecd, g_vecf, opt_m, opt_v, master, tok_ids, act_in):
        shapes = [g.shape[1:] for g in (g_emb, g_attn, g_in, g_out, g_vecd, g_vecf)]
        grads = (tiled(g_emb, 256), tiled(g_attn, 256), tiled(g_in, 1024), tiled(g_out, 256),
                 g_vecd.transpose(1, 2, 0, 3).reshape(27, 1, 256), g_vecf.reshape(24, 128))
        state = [s.reshape(SHARD, 128) for s in (opt_m, opt_v, master)]
        anywhere = pl.BlockSpec(memory_space=pltpu.HBM)
        vmem = pl.BlockSpec(memory_space=pltpu.VMEM)
        slots = pltpu.VMEM((3, 4, 16, PART, 128), F32)
        dma = pltpu.SemaphoreType.DMA
        shard = pltpu.VMEM((SHARD, 128), F32)
        m_new, v_new, w_new, flat = pl.pallas_call(
            sync_kernel,
            name="sync",
            out_shape=(shard, shard, shard, pltpu.VMEM((ROWS, 128), F32)),
            in_specs=[anywhere] * 6 + [vmem] * 3,
            out_specs=[vmem] * 4,
            scratch_shapes=[pltpu.VMEM(g.shape, F32) for g in grads] + [
                pltpu.VMEM((3, 2, 64, APART, 128), BF16), slots, slots, slots,
                pltpu.VMEM((3, 4, 6, 2, PART, 128), F32),
                pltpu.VMEM((3, 6, 2, PART, 128), F32),
                pltpu.VMEM((3, 3, PART, 128), F32),
                dma((6,)), dma((3, 4, 4)), dma((3, 4, 4)), dma((3, 4, 6)), dma((3, 4, 6)),
                dma((3, 6)), dma((3, 6)), dma((3, 3)), dma((3, 3)),
                dma((3, 3)), dma((3, 3)), dma((3, 4, 3)), dma((3, 4, 3)),
                dma((3, 4, 4)), dma((3, 4, 4)), dma((3, 4, 4)), dma((3, 4, 4))],
            compiler_params=pltpu.CompilerParams(
                collective_id=0, has_side_effects=True, vmem_limit_bytes=50 * 1048576),
        )(*grads, *state)

        staged = [(2048, 256), (3072, 256), (768, 1024), (3072, 256), (9, 3, 256), (3, 1024)]
        state_out = jax.ShapeDtypeStruct((SHARD, 128), F32)
        outs = pl.pallas_call(
            apply_kernel,
            name="apply",
            out_shape=[jax.ShapeDtypeStruct(s, BF16) for s in staged + [(256, 256)]] + [state_out] * 3,
            in_specs=[pl.BlockSpec(memory_space=pltpu.SMEM)] + [vmem] * 5,
            out_specs=[anywhere] * 6 + [vmem] + [anywhere] * 3,
            scratch_shapes=[pltpu.VMEM(s, BF16) for s in staged] + [
                pltpu.VMEM((512, 128), F32), dma((9,))],
            compiler_params=pltpu.CompilerParams(vmem_limit_bytes=24 * 1048576),
        )(tok_ids, flat, act_in, m_new, v_new, w_new)
        halves = [o.reshape(s) for o, s in zip(outs[:4], shapes)]
        halves += [outs[4].transpose(1, 0, 2), outs[5]]
        return (*[o.reshape(-1) for o in outs[7:]], *halves, outs[6])

    grad_specs = tuple(P(AXES, *([None] * (grad_rank - 1))) for grad_rank in GRAD_RANKS)
    in_specs = grad_specs + (P(AXES), P(AXES), P(AXES), P(AXES), P(AXES, None))
    out_specs = (P(AXES), P(AXES), P(AXES), P(), P(), P(), P(), P(), P(), P(AXES, None))
    return jax.shard_map(device_step, mesh=mesh, in_specs=in_specs, out_specs=out_specs, check_vma=False)
```

```python
import functools
import math
import jax
import jax.numpy as jnp
from jax import lax
from jax.experimental import pallas as pl
from jax.experimental.pallas import tpu as pltpu
from jax.sharding import PartitionSpec as P

LEARN_RATE = 0.002
BETA_ONE = 0.9
BETA_TWO = 0.95
ADAM_EPS = 1e-8
ADAM_STEP = 2
AXES = ("dz", "dy", "dx")
GRAD_RANKS = (3, 5, 4, 4, 4, 3)
MESH = pl.DeviceIdType.MESH

SHARD = 177
RING = 4
LANES = 128
DEVICES = 128
PART = 59
APART = 60
ROWS = 22656
REAL = 22606
BASE = (0, 4096, 10240, 16384, 22528, 22582)
GROUPS = (256, 384, 96, 384)
TILES = (2, 2, 8, 2)
ORDER = ((0, 1, 2), (1, 2, 0), (2, 0, 1))
F32 = jnp.float32
BF16 = jnp.bfloat16


def loop(count, body, unroll=1):
    def step(i, carry):
        body(i)
        return carry
    lax.fori_loop(0, count, step, 0, unroll=unroll)


def shard_of(k, q1, q2, q3, core):
    pos = [None] * 3
    for axis, q in zip(ORDER[k], (q1, q2, q3)):
        pos[axis] = q
    return pos[2] * 32 + pos[1] * 8 + pos[0] * 2 + core


def sync_kernel(e_hbm, a_hbm, i_hbm, o_hbm, vd_hbm, vf_hbm, m_ref, v_ref, w_ref,
                m_out, v_out, w_out, flat,
                e_raw, a_raw, i_raw, o_raw, vd_raw, vf_raw, ag, psl, work, drx,
                r1, r2, r3,
                raw_sem, sent, drecv, s1recv, s2recv, s3recv, g2recv, g1recv, g0recv, shrecv):
    dz, dy, dx = lax.axis_index("dz"), lax.axis_index("dy"), lax.axis_index("dx")
    core = lax.rem(dx, 2)
    pos = (lax.div(dx, 2), dy, dz)
    partner = {"dz": dz, "dy": dy, "dx": dx + 1 - 2 * core}
    colours = range(3)
    FAR = (2, 1, -1, 0)

    def neighbour(axis, shift):
        q = lax.rem(pos[axis] + RING + shift, RING)
        if axis == 0:
            return {"dz": dz, "dy": dy, "dx": q * 2 + core}
        if axis == 1:
            return {"dz": dz, "dy": q, "dx": dx}
        return {"dz": q, "dy": dy, "dx": dx}

    def ring(axis, shift):
        return lax.rem(pos[axis] + RING + shift, RING)

    def remote(src, dst, send_sem, recv_sem, device):
        return pltpu.make_async_remote_copy(
            src_ref=src, dst_ref=dst, send_sem=send_sem, recv_sem=recv_sem,
            device_id=device, device_id_type=MESH)

    def arrive(sem, like, name):
        with jax.named_scope(name):
            pltpu.make_async_copy(like, like, sem).wait()

    def slots_like(count):
        return ag.at[:, 0, pl.ds(0, count)]

    barrier = pltpu.get_barrier_semaphore()
    for axis in range(3):
        for shift in (1, -1, 2):
            pl.semaphore_signal(barrier, inc=1, device_id=neighbour(axis, shift), device_id_type=MESH)
    pl.semaphore_signal(barrier, inc=1, device_id=partner, device_id_type=MESH)

    raws = (e_raw, a_raw, i_raw, o_raw, vd_raw, vf_raw)
    loads = [pltpu.make_async_copy(src, dst, raw_sem.at[n]) for n, (src, dst) in enumerate(
        zip((e_hbm, a_hbm, i_hbm, o_hbm, vd_hbm, vf_hbm), raws))]
    for load in loads:
        load.start()

    flat[pl.ds(REAL, ROWS - REAL), :] = jnp.zeros((ROWS - REAL, LANES), F32)
    for n in range(RING):
        with jax.named_scope(f"load{n}"):
            loads[n].wait()
        tiles, base, raw = TILES[n], BASE[n], raws[n]

        def relayout(g, tiles=tiles, base=base, raw=raw):
            for c in range(tiles):
                flat[pl.ds(base + g * (8 * tiles) + c, 8, stride=tiles), :] = raw[g, c]
        loop(GROUPS[n], relayout, unroll=16 // tiles)
    loads[4].wait()
    for i in range(27):
        for h in range(2):
            flat[pl.ds(BASE[4] + 2 * i + h, 1), :] = vd_raw[i, :, LANES * h:LANES * h + LANES]
    loads[5].wait()
    flat[pl.ds(BASE[5], 24), :] = vf_raw[...]

    with jax.named_scope("enter"):
        pl.semaphore_wait(barrier, 10)

    def d2d(k, i1, i2):
        q1, q2 = ring(ORDER[k][0], FAR[i1]), ring(ORDER[k][1], FAR[i2])
        at = (k, q1, pl.ds(RING * q2, 4))
        return remote(psl.at[at], drx.at[at], sent.at[0], drecv.at[RING * i2 + i1], partner)

    for i2 in range(RING):
        for i1 in range(RING):
            for k in colours:
                q1, q2 = ring(ORDER[k][0], FAR[i1]), ring(ORDER[k][1], FAR[i2])

                def pick(j, k=k, q1=q1, q2=q2):
                    row = SHARD * shard_of(k, q1, q2, j, 1 - core) + PART * k
                    psl[k, q1, RING * q2 + j] = flat[pl.ds(row, PART), :]
                loop(RING, pick, unroll=2)
                d2d(k, i1, i2).start()

    def add_core(i1, i2):
        arrive(drecv.at[RING * i2 + i1], drx.at[:, 0, pl.ds(0, RING)], f"d{i2}_{i1}")
        for k in colours:
            q1, q2 = ring(ORDER[k][0], FAR[i1]), ring(ORDER[k][1], FAR[i2])

            def body(j, k=k, q1=q1, q2=q2):
                row = SHARD * shard_of(k, q1, q2, j, core) + PART * k
                work[k, q1, RING * q2 + j] = flat[pl.ds(row, PART), :] + drx[k, q1, RING * q2 + j]
            loop(RING, body, unroll=2)

    PARTS = ((2, 0, 1), (2, 1, -1), (1, 1, 1), (1, 0, 1), (-1, 0, -1), (-1, 1, -1))

    ADDS = ((1, 0), (-1, 1), (0, 1), (0, 0), (0, 0), (0, 1))

    def chunk(k, s1, s2, half):
        q1, q2 = ring(ORDER[k][0], s1), ring(ORDER[k][1], s2)
        return work.at[k, q1, pl.ds(RING * q2 + 2 * half, 2)]

    def own3(k, shift):
        q1, q2, q3 = ring(ORDER[k][0], 0), ring(ORDER[k][1], 0), ring(ORDER[k][2], shift)
        return work.at[k, q1, RING * q2 + q3]

    def rs1(i2, *parts):
        for k in colours:
            for part in parts:
                shift, half, way = PARTS[part]
                remote(chunk(k, shift, FAR[i2], half), r1.at[k, i2, part],
                       sent.at[1], s1recv.at[6 * i2 + part], neighbour(ORDER[k][0], way)).start()

    def rs2(*parts):
        for k in colours:
            for part in parts:
                shift, half, way = PARTS[part]
                remote(chunk(k, 0, shift, half), r2.at[k, part],
                       sent.at[2], s2recv.at[part], neighbour(ORDER[k][1], way)).start()

    def add1(i2, part):
        arrive(s1recv.at[6 * i2 + part], r1.at[:, i2, part], f"a{i2}_{part}")
        shift, half = ADDS[part]
        for k in colours:
            dst = chunk(k, shift, FAR[i2], half)
            dst[...] = dst[...] + r1[k, i2, part]

    def add2(part):
        arrive(s2recv.at[part], r2.at[:, part], f"b{part}")
        shift, half = ADDS[part]
        for k in colours:
            dst = chunk(k, 0, shift, half)
            dst[...] = dst[...] + r2[k, part]

    def first(i2):
        add_core(0, i2)
        rs1(i2, 0, 1)
        add_core(1, i2)
        rs1(i2, 2)
        add_core(2, i2)
        rs1(i2, 4)

    def relay(i2):
        add1(i2, 0)
        rs1(i2, 3)
        add1(i2, 1)
        rs1(i2, 5)

    def finish(i2):
        add_core(3, i2)
        for part in (2, 4, 3, 5):
            add1(i2, part)

    first(0)
    first(1)
    relay(0)
    first(2)
    relay(1)
    finish(0)
    rs2(0, 1)
    first(3)
    relay(2)
    finish(1)
    rs2(2)
    relay(3)
    finish(2)
    rs2(4)
    add2(0)
    rs2(3)
    add2(1)
    rs2(5)
    finish(3)
    for part in (2, 4, 3, 5):
        add2(part)
    for k in colours:
        for i3 in colours:
            remote(own3(k, FAR[i3]), r3.at[k, i3], sent.at[3], s3recv.at[0],
                   neighbour(ORDER[k][2], FAR[i3])).start()

    arrive(s3recv.at[0], r3, "c")
    for k in colours:
        rows = pl.ds(PART * k, PART)
        grad = own3(k, 0)[...] + r3[k, 0] + r3[k, 1] + r3[k, 2]
        grad = grad * (1.0 / DEVICES)
        m_new = BETA_ONE * m_ref[rows, :] + (1.0 - BETA_ONE) * grad
        v_new = BETA_TWO * v_ref[rows, :] + (1.0 - BETA_TWO) * grad * grad
        m_hat = m_new / (1.0 - BETA_ONE ** ADAM_STEP)
        v_hat = v_new / (1.0 - BETA_TWO ** ADAM_STEP)
        m_out[rows, :] = m_new
        v_out[rows, :] = v_new
        w_out[rows, :] = w_ref[rows, :] - LEARN_RATE * m_hat / (jnp.sqrt(v_hat) + ADAM_EPS)

    def slot(k, s1, s2, s3):
        axes = ORDER[k]
        return 16 * ring(axes[0], s1) + RING * ring(axes[1], s2) + ring(axes[2], s3)

    for k in colours:
        own = slot(k, 0, 0, 0)
        if k < 2:
            ag[k, core, own] = w_out[pl.ds(APART * k, APART), :].astype(BF16)
        else:
            vals = jnp.concatenate([w_out[pl.ds(120, 57), :], jnp.zeros((3, LANES), F32)], axis=0)
            ag[k, core, own] = vals.astype(BF16)

    def unpack(c, i1, i2):
        for k in colours:
            q1, q2 = ring(ORDER[k][0], NEAR[i1]), ring(ORDER[k][1], NEAR[i2])
            size = APART if k < 2 else 57

            def body(j, k=k, q1=q1, q2=q2, size=size):
                row = SHARD * shard_of(k, q1, q2, j, c) + APART * k
                flat[pl.ds(row, size), :] = ag[k, c, 16 * q1 + RING * q2 + j].astype(F32)[:size]
            loop(RING, body, unroll=2)

    NEAR = (0, -1, 1, 2)

    WAYS = (1, -1, 2)

    def g2(i):
        for k in colours:
            ref = ag.at[k, core, slot(k, 0, 0, 0)]
            remote(ref, ref, sent.at[4], g2recv.at[i], neighbour(ORDER[k][2], WAYS[i])).start()

    ONWARD = (1, -1, -1, 1)

    def g1(i3, part):
        way = (*WAYS, ONWARD[i3])[part if part < 2 else 3]
        start = -ONWARD[i3] if part == 2 else 0
        for k in colours:
            ref = ag.at[k, core, slot(k, 0, start, NEAR[i3])]
            remote(ref, ref, sent.at[5], g1recv.at[3 * i3 + part], neighbour(ORDER[k][1], way)).start()

    def got1(i3, part):
        arrive(g1recv.at[3 * i3 + part], slots_like(1), f"e{i3}_{part}")

    def g0(i2, part):
        way = (1, -1)[part % 2]
        start = -way if part > 1 else 0
        for k in colours:
            at = slot(k, start, NEAR[i2], 0) - ring(ORDER[k][2], 0)
            if part > 1:
                ref = ag.at[k, core, pl.ds(at + 2 * (part - 2), 2)]
            else:
                ref = ag.at[k, core, pl.ds(at, RING)]
            remote(ref, ref, sent.at[6], g0recv.at[RING * i2 + part], neighbour(ORDER[k][0], way)).start()

    def got0(i2, part):
        arrive(g0recv.at[RING * i2 + part], slots_like(2 if part > 1 else 4), f"f{i2}_{part}")

    def give(i1, i2):
        for k in colours:
            at = slot(k, NEAR[i1], NEAR[i2], 0) - ring(ORDER[k][2], 0)
            ref = ag.at[k, core, pl.ds(at, RING)]
            remote(ref, ref, sent.at[7], shrecv.at[RING * i1 + i2], partner).start()

    def take(i1, *places):
        for i2 in places:
            arrive(shrecv.at[RING * i1 + i2], slots_like(RING), f"s{i1}_{i2}")
            unpack(1 - core, i1, i2)

    def mine(i1, *places):
        for i2 in places:
            unpack(core, i1, i2)

    def group(i2):
        g0(i2, 0)
        g0(i2, 1)
        give(0, i2)

    def onward0(i2):
        for part in range(2):
            got0(i2, part)
            g0(i2, part + 2)
            give(part + 1, i2)

    def last0(i2):
        got0(i2, 2)
        got0(i2, 3)
        give(3, i2)

    for i in colours:
        g2(i)
    g1(0, 0)
    g1(0, 1)
    for i in colours:
        arrive(g2recv.at[i], slots_like(1), f"h{i}")
        g1(i + 1, 0)
        g1(i + 1, 1)
    group(0)
    mine(0, 0)
    for i3 in range(RING):
        for part in range(2):
            got1(i3, part)
            if WAYS[part] == ONWARD[i3]:
                g1(i3, 2)
    group(1)
    group(2)
    onward0(0)
    for i3 in range(RING):
        got1(i3, 2)
    group(3)
    mine(0, 1, 2, 3)
    take(0, 0)
    onward0(1)
    onward0(2)
    for i1 in (1, 2):
        mine(i1, 0)
    take(0, 1, 2)
    last0(0)
    for i1 in (1, 2):
        mine(i1, 1, 2)
        take(i1, 0)
    mine(3, 0)
    take(0, 3)
    onward0(3)
    last0(1)
    last0(2)
    mine(3, 1, 2)
    for i1 in (1, 2):
        mine(i1, 3)
        take(i1, 1, 2)
    take(3, 0)
    last0(3)
    mine(3, 3)
    take(3, 1, 2)
    for i1 in (1, 2, 3):
        take(i1, 3)

    for n, like in enumerate((psl, r1, r2, r3, slots_like(3), slots_like(12), slots_like(48), slots_like(64))):
        arrive(sent.at[n], like, f"sent{n}")


def apply_kernel(ids, flat, act, m_in, v_in, w_in,
                 emb_out, attn_out, in_out, ff_out, vd_out, vf_out, y_out, m_out, v_out, w_out,
                 emb_v, attn_v, in_v, out_v, vd_v, vf_v, rows_v, sems):
    copies = []

    def send(src, dst):
        copy = pltpu.make_async_copy(src, dst, sems.at[len(copies)])
        copy.start()
        copies.append(copy)

    for src, dst in ((m_in, m_out), (v_in, v_out), (w_in, w_out)):
        send(src, dst)
    stage = (emb_v, attn_v, in_v, out_v)
    outs = (emb_out, attn_out, in_out, ff_out)
    for n in range(RING):
        tiles, base, dst = TILES[n], BASE[n], stage[n]

        def pack(g, tiles=tiles, base=base, dst=dst):
            rows = pl.ds(pl.multiple_of(16 * g, 16), 16)
            for c in range(tiles):
                vals = flat[pl.ds(base + g * (16 * tiles) + c, 16, stride=tiles), :]
                dst[rows, LANES * c:LANES * c + LANES] = vals.astype(BF16)
        loop(GROUPS[n] // 2, pack, unroll=8 // tiles)
        send(dst, outs[n])
    for r in range(9):
        for h in range(2):
            vals = flat[pl.ds(BASE[4] + 2 * r + h, 3, stride=18), :]
            vd_v[r, :, LANES * h:LANES * h + LANES] = vals.astype(BF16)
    for c in range(8):
        vf_v[:, LANES * c:LANES * c + LANES] = flat[pl.ds(BASE[5] + c, 3, stride=8), :].astype(BF16)
    send(vd_v, vd_out)
    send(vf_v, vf_out)

    def look(i):
        rows_v[pl.ds(2 * i, 2), :] = flat[pl.ds(2 * ids[i], 2), :]
    loop(256, look, unroll=8)

    def bias(row, count):
        flat_vals = flat[pl.ds(row, count), :].astype(BF16).astype(F32)
        return jnp.concatenate([flat_vals[i:i + 1] for i in range(count)], axis=1)
    emb = jnp.concatenate([rows_v[pl.ds(0, 256, stride=2), :], rows_v[pl.ds(1, 256, stride=2), :]], axis=1)
    hidden = (emb * 16.0 + act[...].astype(F32)).astype(BF16)
    pre = jnp.dot(hidden, in_v[0:256, :], preferred_element_type=F32) + bias(BASE[5], 8)
    inner = jax.nn.gelu(pre, approximate=True).astype(BF16)
    y = jnp.dot(inner, out_v[0:1024, :], preferred_element_type=F32) + bias(BASE[4] + 16, 2)
    y_out[...] = y.astype(BF16)
    for copy in copies:
        copy.wait()


def tiled(grad, width):
    flat = grad.reshape(-1, 8, width // LANES, LANES)
    return flat.transpose(0, 2, 1, 3)


def solution(mesh):
    def device_step(g_emb, g_attn, g_in, g_out, g_vecd, g_vecf, opt_m, opt_v, master, tok_ids, act_in):
        shapes = [g.shape[1:] for g in (g_emb, g_attn, g_in, g_out, g_vecd, g_vecf)]
        grads = (tiled(g_emb, 256), tiled(g_attn, 256), tiled(g_in, 1024), tiled(g_out, 256),
                 g_vecd.transpose(1, 2, 0, 3).reshape(27, 1, 256), g_vecf.reshape(24, LANES))
        state = [s.reshape(SHARD, LANES) for s in (opt_m, opt_v, master)]
        anywhere = pl.BlockSpec(memory_space=pltpu.HBM)
        vmem = pl.BlockSpec(memory_space=pltpu.VMEM)
        slots = pltpu.VMEM((3, 4, 16, PART, LANES), F32)
        dma = pltpu.SemaphoreType.DMA
        shard = pltpu.VMEM((SHARD, LANES), F32)
        m_new, v_new, w_new, flat = pl.pallas_call(
            sync_kernel,
            name="sync",
            out_shape=(shard, shard, shard, pltpu.VMEM((ROWS, LANES), F32)),
            in_specs=[anywhere] * 6 + [vmem] * 3,
            out_specs=[vmem] * 4,
            scratch_shapes=[pltpu.VMEM(g.shape, F32) for g in grads] + [
                pltpu.VMEM((3, 2, 64, APART, LANES), BF16), slots, slots, slots,
                pltpu.VMEM((3, 4, 6, 2, PART, LANES), F32),
                pltpu.VMEM((3, 6, 2, PART, LANES), F32),
                pltpu.VMEM((3, 3, PART, LANES), F32),
                *[dma((n,)) for n in (6, 8, 16, 24, 6, 1, 3, 12, 16, 16)]],
            compiler_params=pltpu.CompilerParams(
                collective_id=0, has_side_effects=True, vmem_limit_bytes=50 * 1048576),
        )(*grads, *state)

        staged = [(math.prod(s[:-1]), s[-1]) for s in shapes[:4]] + [(9, 3, 256), shapes[5]]
        state_out = jax.ShapeDtypeStruct((SHARD, LANES), F32)
        outs = pl.pallas_call(
            apply_kernel,
            name="apply",
            out_shape=[jax.ShapeDtypeStruct(s, BF16) for s in staged + [(256, 256)]] + [state_out] * 3,
            in_specs=[pl.BlockSpec(memory_space=pltpu.SMEM)] + [vmem] * 5,
            out_specs=[anywhere] * 6 + [vmem] + [anywhere] * 3,
            scratch_shapes=[pltpu.VMEM(s, BF16) for s in staged] + [
                pltpu.VMEM((512, LANES), F32), dma((9,))],
            compiler_params=pltpu.CompilerParams(vmem_limit_bytes=24 * 1048576),
        )(tok_ids, flat, act_in, m_new, v_new, w_new)
        halves = [o.reshape(s) for o, s in zip(outs[:4], shapes)]
        halves += [outs[4].transpose(1, 0, 2), outs[5]]
        return (*[o.reshape(-1) for o in outs[7:]], *halves, outs[6])

    grad_specs = tuple(P(AXES, *([None] * (grad_rank - 1))) for grad_rank in GRAD_RANKS)
    in_specs = grad_specs + (P(AXES), P(AXES), P(AXES), P(AXES), P(AXES, None))
    out_specs = (P(AXES), P(AXES), P(AXES), P(), P(), P(), P(), P(), P(), P(AXES, None))
    return jax.shard_map(device_step, mesh=mesh, in_specs=in_specs, out_specs=out_specs, check_vma=False)
```
